32 devices in a mesh: dp: 8 (over z, y), fsdp: 4 (over x, core).
Axes of the slice: x: 2, y: 2, z: 4, core: 2. Of those that a mesh axis runs over, the one named last changes fastest.
Arguments:
- momentum: float32 [2, 6144, 16384], P(None, 'fsdp', 'dp'), may hold values from -160 to 160, as said below
- gradient: bfloat16 [2, 6144, 16384], P(None, 'fsdp', 'dp'), may hold values from -6 to 6
- q_factor: float32 [2, 16384, 256], P(None, 'dp'), may hold values from -6 to 6
Outputs:
- new_momentum: float32 [2, 6144, 16384], P(None, 'fsdp', 'dp')
- update: bfloat16 [2, 6144, 16384], P(None, 'fsdp', 'dp')
- new_q: float32 [2, 16384, 256], P(None, 'dp')
The draws below stay inside these ranges and needn't reach their ends.
Inputs may be any that keep to these rules, and one draw needn't show every extreme that they name: `momentum`: Real-valued entries.
All inputs are finite; a program needn't handle non-finite values.
Results may differ from the reference program's by a relative error of at most 0.001.
Values sent between devices are 32-bit elements; how exact they have to be, the bound alone decides.
A program may use at most 192 MiB of HBM per device.

```python
import jax
import jax.numpy as jnp
from jax import lax

M = 6144
N = 16384
R = 256
E = 2


def draw_momentum(key, part):
    random_key, row_key, col_key = jax.random.split(key, 3)
    row_place = jnp.arange(M, dtype=jnp.float32) / M - 0.5
    col_place = jnp.arange(N, dtype=jnp.float32) / N - 0.5
    random_part = jax.random.truncated_normal(random_key, -5.0, 5.0, (E, M, N), jnp.float32)
    spread = 1.15
    growth = 3.0
    row_scale = jnp.exp(row_place[None, :, None] * jnp.log(growth) + jax.random.uniform(row_key, (E, M, 1), jnp.float32, -spread, spread))
    col_scale = jnp.exp(col_place[None, None, :] * jnp.log(growth) + jax.random.uniform(col_key, (E, 1, N), jnp.float32, -spread, spread))
    return random_part * row_scale * col_scale


def steps_of(own_key, extent, cuts, low, top_value):
    loudness = 1.0
    for axis_at, parts in cuts:
        draws = jax.random.uniform(jax.random.fold_in(jax.random.fold_in(own_key, 6), axis_at), (parts,), jnp.float32, low / len(cuts), top_value / len(cuts))
        loudness = loudness * jnp.repeat(jnp.exp(draws), extent[axis_at] // parts).reshape((-1,) + (1,) * (len(extent) - 1 - axis_at))
    return loudness


def gaussian(key, shape, scale, limit, cuts=(), kind=jnp.bfloat16):
    factor_of = steps_of(key, shape, cuts, -0.22, 0.18) if cuts else 1.0
    drawn = jax.random.normal(key, shape, jnp.float32) * scale * factor_of
    return jnp.minimum(jnp.maximum(drawn, -limit), limit).astype(kind)


def setup_inputs(seed: int = 0) -> dict:
    arg_keys = jax.random.split(jax.random.key(seed), 4)
    momentum = draw_momentum(jax.random.fold_in(arg_keys[3], 71), 0)
    gradient = gaussian(arg_keys[1], (E, M, N), 1.0, 6.0, ((1, 4), (2, 8)))
    q_factor = gaussian(arg_keys[2], (E, N, R), 1.0, 6.0, ((1, 8),), jnp.float32)
    return {"momentum": momentum, "gradient": gradient, "q_factor": q_factor}


ema_decay = 0.75
epsilon = 1e-06

def one_matrix(inputs):
    moment_part, grad_part, q_part = inputs
    buffer = moment_part + grad_part.astype(jnp.float32)
    left = jnp.dot(buffer, q_part, precision=lax.Precision.HIGHEST)
    gram_matrix = jnp.dot(left.T, left, precision=lax.Precision.HIGHEST)
    lower_factor = jnp.linalg.cholesky(gram_matrix)
    orthonormal = lax.linalg.triangular_solve(lower_factor, left, left_side=False, lower=True, transpose_a=True)
    right_factor = jnp.dot(buffer.T, orthonormal, precision=lax.Precision.HIGHEST)
    new_moment = buffer - (1.0 - ema_decay) * jnp.dot(orthonormal, right_factor.T, precision=lax.Precision.HIGHEST)
    mean_square = lax.optimization_barrier(jnp.mean(right_factor * right_factor, axis=0))
    next_q = right_factor * lax.rsqrt(mean_square + epsilon)[None, :]
    direction = jnp.dot(orthonormal, next_q.T, precision=lax.Precision.HIGHEST) * jnp.sqrt(jnp.float32(M) / jnp.float32(R))
    return (new_moment, direction.astype(jnp.bfloat16), next_q)

def reference(momentum, gradient, q_factor):
    new_momentum, update, new_q = lax.map(one_matrix, (momentum, gradient, q_factor))
    return (new_momentum, update, new_q)
```

```python
import functools
import math

import jax
import jax.numpy as jnp
from jax import lax
from jax.experimental import pallas as pl
from jax.experimental.pallas import tpu as pltpu
from jax.sharding import PartitionSpec as P

MESH = pl.DeviceIdType.MESH
F32 = jnp.float32
BF16 = jnp.bfloat16

ema_decay = 0.75
epsilon = 1e-06
BLOCK = 128
FULL = lax.Precision.HIGHEST
THREE = lax.Precision.HIGH
ONE = lax.Precision.DEFAULT


def inverse_factor_kernel(gram_ref, out_ref, work_left, work_right):
    matrices, size, _ = gram_ref.shape
    rows = lax.broadcasted_iota(jnp.int32, (size, 1), 0)
    lanes = lax.broadcasted_iota(jnp.int32, (1, size), 1)
    eye = jnp.where(rows == lanes, 1.0, 0.0).astype(jnp.float32)
    for e in range(matrices):
        work_left[e] = gram_ref[e]
        work_right[e] = eye

    def step(k, carry):
        for e in range(matrices):
            left = work_left[e]
            right = work_right[e]
            row_left = work_left[e, pl.ds(k, 1), :]
            row_right = work_right[e, pl.ds(k, 1), :]
            pivot = jnp.sum(jnp.where(lanes == k, row_left, 0.0), axis=1, keepdims=True)
            inverse = lax.rsqrt(pivot)
            row_left = row_left * inverse
            row_right = row_right * inverse
            column = jnp.sum(jnp.where(lanes == k, left, 0.0), axis=1, keepdims=True)
            column = jnp.where(rows > k, column * inverse, 0.0)
            work_left[e] = left - column * row_left
            work_right[e] = jnp.where(rows == k, row_right, right - column * row_right)
        return carry

    lax.fori_loop(0, size, step, 0)
    for e in range(matrices):
        out_ref[e] = work_right[e]


def inverse_factor(gram):
    matrices, size, _ = gram.shape
    if size > BLOCK:
        half = size // 2
        top = inverse_factor(gram[:, :half, :half])
        low = jnp.einsum("eij,ekj->eik", gram[:, half:, :half], top, precision=FULL)
        rest = gram[:, half:, half:] - jnp.einsum("eij,ekj->eik", low, low, precision=FULL)
        bottom = inverse_factor(rest)
        cross = -jnp.einsum(
            "eij,ejk->eik", bottom, jnp.einsum("eij,ejk->eik", low, top, precision=FULL), precision=FULL
        )
        zero = jnp.zeros_like(cross).swapaxes(1, 2)
        return jnp.concatenate(
            [jnp.concatenate([top, zero], 2), jnp.concatenate([cross, bottom], 2)], 1
        )
    return pl.pallas_call(
        inverse_factor_kernel,
        out_shape=jax.ShapeDtypeStruct(gram.shape, jnp.float32),
        in_specs=[pl.BlockSpec(memory_space=pltpu.VMEM)],
        out_specs=pl.BlockSpec(memory_space=pltpu.VMEM),
        scratch_shapes=[pltpu.VMEM((matrices, size, size), jnp.float32)] * 2,
        cost_estimate=pl.CostEstimate(
            flops=size * size * size * 4 * matrices, bytes_accessed=8 * size * size * matrices, transcendentals=0
        ),
        name="inverse_factor",
    )(gram)


def swap(value, axis, mask):
    size = lax.axis_size(axis)
    return lax.ppermute(value, axis, [(i, i ^ mask) for i in range(size)])


def levels_of(size):
    return [(1, 0) if i == 0 else ((2 << i) - 2, i) for i in range(size.bit_length() - 1)]


def side_of(index, bit):
    if bit == 0:
        return index & 1
    return ((index >> bit) ^ (index >> (bit + 1))) & 1


def keep_half(value, axis, mask, side):
    half = value.shape[0] // 2
    own = lax.dynamic_slice_in_dim(value, side * half, half, 0)
    other = lax.dynamic_slice_in_dim(value, (1 - side) * half, half, 0)
    return own + swap(other, axis, mask)


def both_halves(value, axis, mask, side):
    other = swap(value, axis, mask)
    return jnp.where(
        side == 0, jnp.concatenate([value, other], 0), jnp.concatenate([other, value], 0)
    )


def sum_halving(value, axis, levels):
    index = lax.axis_index(axis)
    for mask, bit in levels:
        value = keep_half(value, axis, mask, side_of(index, bit))
    for mask, bit in reversed(levels):
        value = both_halves(value, axis, mask, side_of(index, bit))
    return value


def sum_doubling(value, axis, levels):
    for mask, _ in levels:
        value = value + swap(value, axis, mask)
    return value


def sum_near_first(value, axis, levels):
    index = lax.axis_index(axis)
    mask, bit = levels[0]
    side = side_of(index, bit)
    value = keep_half(value, axis, mask, side)
    value = sum_doubling(value, axis, levels[1:])
    return both_halves(value, axis, mask, side)


def general_body(momentum, gradient, q_factor):
    matrices, local_rows, local_cols = momentum.shape
    rank_width = q_factor.shape[2]
    total_rows = local_rows * lax.axis_size("fsdp")
    total_cols = local_cols * lax.axis_size("dp")
    dp_levels = levels_of(lax.axis_size("dp"))
    fsdp_levels = levels_of(lax.axis_size("fsdp"))
    buffers = [momentum[e] + gradient[e].astype(jnp.float32) for e in range(matrices)]
    lefts, grams, rights = [], [], []
    for e in range(matrices):
        partial_value = jnp.einsum("cn,nr->cr", buffers[e], q_factor[e], precision=THREE)
        order = dp_levels if e % 2 == 0 else dp_levels[1:2] + dp_levels[:1] + dp_levels[2:]
        left = sum_halving(partial_value, "dp", order)
        gram = jnp.einsum("cr,ck->rk", left, left, precision=FULL)
        lefts.append(left)
        grams.append(sum_doubling(gram, "fsdp", fsdp_levels))
        right_raw = jnp.einsum("cn,cr->nr", buffers[e], left, precision=THREE)
        rights.append(sum_near_first(right_raw, "fsdp", fsdp_levels))
    inverse = inverse_factor(jnp.stack(grams))
    orthos = [jnp.einsum("cr,kr->ck", lefts[e], inverse[e], precision=FULL) for e in range(matrices)]
    factors = [jnp.einsum("nr,kr->nk", rights[e], inverse[e], precision=FULL) for e in range(matrices)]
    squares = jnp.stack([jnp.sum(f * f, axis=0) for f in factors])
    squares = sum_doubling(squares, "dp", dp_levels)
    col_scale = lax.rsqrt(squares / total_cols + epsilon)
    rms = jnp.sqrt(jnp.float32(total_rows) / jnp.float32(rank_width))
    momenta, updates, new_qs = [], [], []
    for e in range(matrices):
        feedback = jnp.einsum("cr,nr->cn", orthos[e], factors[e], precision=ONE)
        momenta.append(buffers[e] - (1.0 - ema_decay) * feedback)
        new_q = factors[e] * col_scale[e][None, :]
        new_qs.append(new_q)
        direction = jnp.einsum("cr,nr->cn", orthos[e] * rms, new_q, precision=THREE)
        updates.append(direction.astype(jnp.bfloat16))
    return (jnp.stack(momenta), jnp.stack(updates), jnp.stack(new_qs))


def split(value):
    high = value.astype(BF16)
    return high, (value - high.astype(F32)).astype(BF16)


def dot(a, b):
    return jnp.dot(a, b, preferred_element_type=F32)


def dot_rows(a, b):
    return lax.dot_general(a, b, (((1,), (1,)), ((), ())), preferred_element_type=F32)


def eliminate(work, size):
    lanes = lax.broadcasted_iota(jnp.int32, (1, size), 1)
    rows = lax.broadcasted_iota(jnp.int32, (size, 1), 0)
    eight = lax.broadcasted_iota(jnp.int32, (8, 1), 0)

    def step(it, carry):
        base = pl.multiple_of(it * 8, 8)
        whole = work[...]
        block = work[pl.ds(base, 8), :]
        columns, pivots = [], []
        for j in range(8):
            here = lanes == base + j
            columns.append(jnp.sum(jnp.where(here, whole[:, :size], 0.0), axis=1, keepdims=True))
            pivots.append(jnp.sum(jnp.where(here, block[:, :size], 0.0), axis=1, keepdims=True))
        scaled, roots = [], []
        for k in range(8):
            root = lax.rsqrt(pivots[k][k : k + 1, :])
            inverse = root * root
            below = jnp.where(eight > k, pivots[k], 0.0)
            row = block[k : k + 1, :] * inverse
            block = block - below * row
            for j in range(k + 1, 8):
                factor = pivots[j][k : k + 1, :] * inverse
                pivots[j] = pivots[j] - below * factor
                columns[j] = columns[j] - columns[k] * factor
            scaled.append(row)
            roots.append(root)
        under = rows >= base + 8
        for k in range(8):
            whole = whole - jnp.where(under, columns[k], 0.0) * scaled[k]
        work[...] = whole
        root = roots[0]
        for k in range(1, 8):
            root = jnp.where(eight == k, roots[k], root)
        work[pl.ds(base, 8), :] = block * root
        return carry

    lax.fori_loop(0, size // 8, step, 0)


class Plan:
    def __init__(self, mesh, momentum, q_factor):
        self.matrices, self.rows, self.cols = momentum.shape
        self.rank = q_factor.shape[2]
        self.half_rank = self.rank // 2
        self.dp, self.fsdp = mesh.shape["dp"], mesh.shape["fsdp"]
        self.pairs = 4
        self.chunk = self.rows // (2 * self.pairs)
        self.half = self.chunk // 2
        self.width = 256
        self.tiles = self.cols // self.width

    def fits(self):
        return (
            self.dp == 8
            and self.fsdp == 4
            and self.rank == 256
            and self.rows % (32 * self.pairs) == 0
            and self.rows % 128 == 0
            and self.cols % (2 * self.width) == 0
            and self.rows % (16 * self.tiles) == 0
            and self.matrices * self.rows * self.cols <= 6 << 20
        )


def factor_kernel(
    plan,
    mom,
    grad,
    q,
    left_out,
    inverse_out,
    fact_out,
    square_out,
    bh,
    bl,
    mst,
    gst,
    qst,
    qh,
    ql,
    left,
    final,
    a_y,
    a_z1,
    a_z2,
    b_z1,
    b_z2,
    b_y,
    turned,
    turned_split,
    own,
    from_core,
    from_x,
    right,
    gram0,
    gram1,
    gram2,
    gram_core,
    gram_x,
    work,
    inverse,
    sq,
    sq_in,
    in_sem,
    q_sem,
    l_send,
    l_recv,
    r_send,
    r_recv,
    g_send,
    g_recv,
    s_send,
    s_recv,
    out_sem,
):
    E, K, H = plan.matrices, plan.rank, plan.half_rank
    NP, CH, HF, W, T = plan.pairs, plan.chunk, plan.half, plan.width, plan.tiles
    R = plan.rows
    d, f = lax.axis_index("dp"), lax.axis_index("fsdp")
    y, z = d % 2, d // 2
    core = f % 2
    mid = jnp.logical_or(z == 1, z == 2)
    leaf = jnp.logical_not(mid)
    zside = z // 2
    y_peer = (z * 2 + 1 - y, f)
    z_peer = ((z + 1 - 2 * (z % 2)) * 2 + y, f)
    m_peer = ((3 - z) * 2 + y, f)
    x_peer = (d, (f + 2) % 4)
    c_peer = (d, f + 1 - 2 * core)

    def remote(src, dst, send, recv, peer):
        return pltpu.make_async_remote_copy(
            src_ref=src, dst_ref=dst, send_sem=send, recv_sem=recv, device_id=peer, device_id_type=MESH
        )

    drains = []

    def start(copy, when=None):
        if when is None:
            copy.start()
        else:
            pl.when(when)(copy.start)
        drains.append((copy, when))

    def load(e, index, slot):
        at = pl.ds(pl.multiple_of(index * CH, CH), CH)
        return (
            pltpu.make_async_copy(mom.at[e, at, :], mst.at[slot], in_sem.at[0, slot]),
            pltpu.make_async_copy(grad.at[e, at, :], gst.at[slot], in_sem.at[1, slot]),
        )

    def load_q(e):
        return pltpu.make_async_copy(q.at[e], qst, q_sem)

    load_q(0).start()
    for slot in range(2):
        for copy in load(0, slot, slot):
            copy.start()

    barrier = pltpu.get_barrier_semaphore()
    for peer in (y_peer, z_peer, m_peer, x_peer, c_peer):
        pl.semaphore_signal(barrier, inc=1, device_id=peer, device_id_type=MESH)

    def left_products(e):
        load_q(e).wait()
        for c in range(0, plan.cols, 256):
            high, low = split(qst[c : c + 256, :])
            qh[c : c + 256, :] = high
            ql[c : c + 256, :] = low
        if e + 1 < E:
            load_q(e + 1).start()

        def pair(p, carry):
            for color in range(2):
                index = p * 2 + color
                at = pl.ds(pl.multiple_of(index * CH, CH), CH)
                for copy in load(e, index, color):
                    copy.wait()
                for c in range(0, plan.cols, 512):
                    cs = slice(c, c + 512)
                    high, low = split(mst[color, :, cs] + gst[color, :, cs].astype(F32))
                    bh[e, at, cs] = high
                    bl[e, at, cs] = low

                @pl.when(p < NP - 1)
                def _():
                    for copy in load(e, index + 2, color):
                        copy.start()

                if e + 1 < E:

                    @pl.when(p == NP - 1)
                    def _():
                        for copy in load(e + 1, color, color):
                            copy.start()

                b_high, b_low = bh[e, at, :], bl[e, at, :]
                total = dot(b_high, qh[...]) + dot(b_low, qh[...]) + dot(b_high, ql[...])
                left[e, 0, at, :] = total[:, :H]
                left[e, 1, at, :] = total[:, H:]
            return carry

        lax.fori_loop(0, NP, pair, 0)

    def rows_of(color, p, part=None):
        base = (2 * p + color) * CH
        if part is None:
            return pl.ds(base, CH)
        return pl.ds(pl.multiple_of(base + part * HF, HF), HF)

    def copies(e, h, p):
        u = (e * 2 + h) * NP + p
        s, r = (lambda i: l_send.at[u, i]), (lambda i: l_recv.at[u, i])
        part = lambda ref, color, which=None: ref.at[e, h, rows_of(color, p, which), :]
        mine, other = part(left, 0, y), part(left, 0, 1 - y)
        done, done_other = part(final, 0, y), part(final, 0, 1 - y)
        zmine, zother = part(left, 1, zside), part(left, 1, 1 - zside)
        zdone, zdone_other = part(final, 1, zside), part(final, 1, 1 - zside)
        return dict(
            a0=remote(other, a_y.at[u], s(0), r(0), y_peer),
            a1=remote(mine, a_z1.at[u], s(1), r(1), z_peer),
            a2=remote(mine, a_z2.at[u], s(1), r(2), m_peer),
            a3=remote(done, done, s(2), r(1), z_peer),
            a4=remote(done, done, s(3), r(3), y_peer),
            a5=remote(done_other, done_other, s(3), r(3), y_peer),
            b0=remote(part(left, 1), b_z1.at[u], s(4), r(4), z_peer),
            b1=remote(zother, b_z2.at[u], s(4), r(5), m_peer),
            b2=remote(zmine, b_y.at[u], s(5), r(6), y_peer),
            b3=remote(zdone, zdone, s(6), r(7), m_peer),
            b3w=remote(zdone_other, zdone_other, s(6), r(7), m_peer),
            b4=remote(zdone, zdone, s(7), r(4), z_peer),
            b5=remote(zdone_other, zdone_other, s(8), r(5), z_peer),
        ), (e, h, p, u)

    table = [copies(e, h, p) for e in range(E) for h in range(2) for p in range(NP)]

    def stage(k, s):
        c, (e, h, p, u) = table[k]
        at = lambda color, part=None: (e, h, rows_of(color, p, part), slice(None))
        if s == 0:
            start(c["a0"])
            start(c["b0"], leaf)
        elif s == 1:
            c["a0"].wait_recv()
            left[at(0, y)] = left[at(0, y)] + a_y[u]
            start(c["a1"], leaf)

            @pl.when(mid)
            def _():
                c["b0"].wait_recv()
                left[at(1)] = left[at(1)] + b_z1[u]

            start(c["b1"], mid)
        elif s == 2:

            @pl.when(mid)
            def _():
                c["a1"].wait_recv()
                left[at(0, y)] = left[at(0, y)] + a_z1[u]
                c["a2"].start()
                c["b1"].wait_recv()
                left[at(1, zside)] = left[at(1, zside)] + b_z2[u]
                c["b2"].start()

            drains.append((c["a2"], mid))
            drains.append((c["b2"], mid))
        elif s == 3:

            @pl.when(mid)
            def _():
                c["a2"].wait_recv()
                final[at(0, y)] = left[at(0, y)] + a_z2[u]
                c["a3"].start()
                c["a4"].start()
                c["b2"].wait_recv()
                final[at(1, zside)] = left[at(1, zside)] + b_y[u]
                c["b3"].start()
                c["b4"].start()

            for name in ("a3", "a4", "b3", "b4"):
                drains.append((c[name], mid))
        elif s == 4:

            @pl.when(leaf)
            def _():
                c["a3"].wait_recv()
                c["a4"].start()

            drains.append((c["a4"], leaf))

            @pl.when(mid)
            def _():
                c["b3w"].wait_recv()
                c["b5"].start()

            drains.append((c["b5"], mid))
        elif s == 5:
            c["a5"].wait_recv()

            @pl.when(leaf)
            def _():
                c["b4"].wait_recv()
                c["b5"].wait_recv()

    def write_left(e, h):
        return pltpu.make_async_copy(final.at[e, h], left_out.at[e, h], out_sem.at[e, h])

    def gram_part(ref, e, h):
        return ref.at[e, h, :, pl.ds(0, H * (h + 1))]

    def gram_copy(e, h, which):
        u = e * 2 + h
        src, dst = ((gram0, gram_core), (gram1, gram_x))[which]
        peer = (c_peer, x_peer)[which]
        return remote(gram_part(src, e, h), gram_part(dst, e, h), g_send.at[u, which], g_recv.at[u, which], peer)

    def gram_first(e, h):
        write_left(e, h).start()
        for c in range(0, R, 128):
            turned[:, c : c + 128] = final[e, h, c : c + 128, :].T
        for j in range(h + 1):
            gram0[e, h, :, j * H : (j + 1) * H] = jnp.dot(
                turned[...], final[e, j], precision=FULL, preferred_element_type=F32
            )
        start(gram_copy(e, h, 0))
        high, low = split(turned[...])
        turned_split[:H, :] = high
        turned_split[H:, :] = low

    def gram_second(e, h):
        gram_copy(e, h, 0).wait_recv()
        w = slice(0, H * (h + 1))
        gram1[e, h, :, w] = gram0[e, h, :, w] + gram_core[e, h, :, w]
        start(gram_copy(e, h, 1))

    def gram_third(e, h):
        gram_copy(e, h, 1).wait_recv()
        w = slice(0, H * (h + 1))
        gram2[e, h, :, w] = gram1[e, h, :, w] + gram_x[e, h, :, w]

    def full(a, b, rows=False):
        if rows:
            return lax.dot_general(
                a, b, (((1,), (1,)), ((), ())), precision=FULL, preferred_element_type=F32
            )
        return jnp.dot(a, b, precision=FULL, preferred_element_type=F32)

    def factorize(e, h):
        eye = jnp.where(
            lax.broadcasted_iota(jnp.int32, (H, H), 0) == lax.broadcasted_iota(jnp.int32, (H, H), 1), 1.0, 0.0
        ).astype(F32)
        if h == 0:
            work[:, :H] = gram2[e, 0, :, :H]
            work[:, H:] = eye
            eliminate(work, H)
            inverse[e, :H, :H] = work[:, H:]
            inverse[e, :H, H:] = jnp.zeros((H, H), F32)
        else:
            top = inverse[e, :H, :H]
            low = full(gram2[e, 1, :, :H], top, rows=True)
            work[:, :H] = gram2[e, 1, :, H:] - full(low, low, rows=True)
            work[:, H:] = eye
            cross = full(low, top)
            eliminate(work, H)
            bottom = work[:, H:]
            inverse[e, H:, H:] = bottom
            inverse[e, H:, :H] = -full(bottom, cross)

    def right_copy(e, h, s, which):
        u = e * 2 + h
        tile, other = 2 * s + core, 2 * s + 1 - core
        hs = pl.ds(h * H, H)
        if which == 0:
            src, dst, peer = own.at[u, other], from_core.at[u, s], c_peer
        elif which == 1:
            src, dst, peer = own.at[u, tile], from_x.at[u, s], x_peer
        else:
            tile = tile if which == 2 else other
            src = dst = right.at[e, tile, hs, :]
            peer, which = c_peer, 2
        return remote(src, dst, r_send.at[u, s, which], r_recv.at[u, s, which], peer)

    def right_products(e, h):
        u = e * 2 + h

        def product(tile):
            at = pl.ds(pl.multiple_of(tile * W, W), W)
            both = dot(turned_split[...], bh[e, :, at])
            own[u, tile] = both[:H] + both[H:] + dot(turned_split[:H, :], bl[e, :, at])

        def forward(s):
            right_copy(e, h, s, 0).wait_recv()
            tile = 2 * s + core
            own[u, tile] = own[u, tile] + from_core[u, s]
            right_copy(e, h, s, 1).start()

        def step(s, carry):
            product(2 * s + 1 - core)
            right_copy(e, h, s, 0).start()
            product(2 * s + core)
            pl.when(s > 0)(lambda: forward(s - 1))
            return carry

        lax.fori_loop(0, T // 2, step, 0)
        forward(T // 2 - 1)
        for s in range(T // 2):
            drains.append((right_copy(e, h, s, 0), None))
            drains.append((right_copy(e, h, s, 1), None))

    def right_sums(e, h):
        u = e * 2 + h
        for s in range(T // 2):
            right_copy(e, h, s, 1).wait_recv()
            tile = 2 * s + core
            right[e, tile, pl.ds(h * H, H), :] = own[u, tile] + from_x[u, s]
            right_copy(e, h, s, 2).start()

    def right_others(e, h):
        for s in range(T // 2):
            right_copy(e, h, s, 3).wait_recv()

    def write_fact(e, j):
        return pltpu.make_async_copy(right.at[e, j], fact_out.at[e, j], out_sem.at[e, 2 + j])

    def write_inverse(e):
        return pltpu.make_async_copy(inverse.at[e], inverse_out.at[e], out_sem.at[e, 2 + T])

    def write_square(e):
        return pltpu.make_async_copy(sq.at[e, 3], square_out.at[e], out_sem.at[e, 3 + T])

    def square_copy(e, r):
        peer = (y_peer, z_peer, m_peer)[r]
        return remote(sq.at[e, r], sq_in.at[e, r], s_send.at[e, r], s_recv.at[e, r], peer)

    def factors(e):
        write_inverse(e).start()
        for s in range(T // 2):
            right_copy(e, 0, s, 2).wait_send()
            right_copy(e, 1, s, 2).wait_send()
        x_high, x_low = split(inverse[e])
        total = jnp.zeros((K, 128), F32)
        for j in range(T):
            high, low = split(right[e, j])
            value = dot(x_high, high) + dot(x_low, high) + dot(x_high, low)
            right[e, j] = value
            write_fact(e, j).start()
            for c in range(0, W, 128):
                total = total + value[:, c : c + 128] * value[:, c : c + 128]
        row = jnp.sum(total.T, axis=0, keepdims=True)
        sq[e, 0] = jnp.broadcast_to(row, (8, K))
        start(square_copy(e, 0))

    def square_round(e, r):
        square_copy(e, r).wait_recv()
        sq[e, r + 1] = sq[e, r] + sq_in[e, r]
        if r < 2:
            start(square_copy(e, r + 1))
        else:
            write_square(e).start()

    left_products(0)
    pl.semaphore_wait(barrier, 5)
    SLOTS, STAGES = len(table), 6
    after = {}
    def add(t, *jobs):
        after.setdefault(t, []).extend(jobs)

    add(1, lambda: left_products(1))
    order = [(e, h) for e in range(E) for h in range(2)]
    for u, (e, h) in enumerate(order):
        t = (u + 1) * NP - 1 + STAGES - 1
        add(t, functools.partial(gram_first, e, h), functools.partial(gram_second, e, h), functools.partial(right_products, e, h))
        add(t + 1, functools.partial(gram_third, e, h))
        add(t + 2, functools.partial(factorize, e, h))
        add(t + 3, functools.partial(right_sums, e, h))
        if h == 1:
            add(t + 4, functools.partial(right_others, e, 0), functools.partial(right_others, e, 1), functools.partial(factors, e))
            for r in range(3):
                add(t + 5 + r, functools.partial(square_round, e, r))
    last = max(after)
    for t in range(max(last + 1, SLOTS + STAGES)):
        for s in reversed(range(STAGES)):
            if 0 <= t - s < SLOTS:
                stage(t - s, s)
        for job in after.get(t, []):
            job()

    for copy, when in drains:
        if when is None:
            copy.wait_send()
        else:
            pl.when(when)(copy.wait_send)
    for e in range(E):
        for h in range(2):
            write_left(e, h).wait()
        for j in range(T):
            write_fact(e, j).wait()
        write_inverse(e).wait()
        write_square(e).wait()


def factor_call(plan, momentum, gradient, q_factor):
    E, R, C, K, H = plan.matrices, plan.rows, plan.cols, plan.rank, plan.half_rank
    NP, CH, HF, W, T = plan.pairs, plan.chunk, plan.half, plan.width, plan.tiles
    U = E * 2 * NP
    any_spec = pl.BlockSpec(memory_space=pl.ANY)
    vmem = pltpu.VMEM
    flops = 14 * E * R * C * K
    return pl.pallas_call(
        functools.partial(factor_kernel, plan),
        out_shape=(
            jax.ShapeDtypeStruct((E, 2, R, H), F32),
            jax.ShapeDtypeStruct((E, K, K), F32),
            jax.ShapeDtypeStruct((E, T, K, W), F32),
            jax.ShapeDtypeStruct((E, 8, K), F32),
        ),
        in_specs=[any_spec] * 3,
        out_specs=(any_spec,) * 4,
        scratch_shapes=[
            vmem((E, R, C), BF16),
            vmem((E, R, C), BF16),
            vmem((2, CH, C), F32),
            vmem((2, CH, C), BF16),
            vmem((C, K), F32),
            vmem((C, K), BF16),
            vmem((C, K), BF16),
            vmem((E, 2, R, H), F32),
            vmem((E, 2, R, H), F32),
            vmem((U, HF, H), F32),
            vmem((U, HF, H), F32),
            vmem((U, HF, H), F32),
            vmem((U, CH, H), F32),
            vmem((U, HF, H), F32),
            vmem((U, HF, H), F32),
            vmem((H, R), F32),
            vmem((K, R), BF16),
            vmem((E * 2, T, H, W), F32),
            vmem((E * 2, T // 2, H, W), F32),
            vmem((E * 2, T // 2, H, W), F32),
            vmem((E, T, K, W), F32),
            vmem((E, 2, H, K), F32),
            vmem((E, 2, H, K), F32),
            vmem((E, 2, H, K), F32),
            vmem((E, 2, H, K), F32),
            vmem((E, 2, H, K), F32),
            vmem((H, K), F32),
            vmem((E, K, K), F32),
            vmem((E, 4, 8, K), F32),
            vmem((E, 3, 8, K), F32),
            pltpu.SemaphoreType.DMA((2, 2)),
            pltpu.SemaphoreType.DMA,
            pltpu.SemaphoreType.DMA((U, 9)),
            pltpu.SemaphoreType.DMA((U, 8)),
            pltpu.SemaphoreType.DMA((E * 2, T // 2, 3)),
            pltpu.SemaphoreType.DMA((E * 2, T // 2, 3)),
            pltpu.SemaphoreType.DMA((E * 2, 2)),
            pltpu.SemaphoreType.DMA((E * 2, 2)),
            pltpu.SemaphoreType.DMA((E, 3)),
            pltpu.SemaphoreType.DMA((E, 3)),
            pltpu.SemaphoreType.DMA((E, T + 4)),
        ],
        compiler_params=pltpu.CompilerParams(
            collective_id=0, has_side_effects=True, vmem_limit_bytes=67043328
        ),
        cost_estimate=pl.CostEstimate(flops=flops, bytes_accessed=6 * E * R * C, transcendentals=0),
        name="dion_factors",
    )(momentum, gradient, q_factor)


def output_kernel(
    rms, total_cols, mom, grad, left, inverse, fact, square, new_mom, update, new_q, fh, fl, xh, xl
):
    tiles, width = fact.shape[1], fact.shape[3]
    step = pl.program_id(1)

    @pl.when(step == 0)
    def _():
        for j in range(tiles):
            high, low = split(fact[0, j])
            fh[j] = high
            fl[j] = low
        high, low = split(inverse[0])
        xh[...] = high
        xl[...] = low

    scale = lax.rsqrt(square[0, 0:1, :] / total_cols + epsilon)
    high, low = split(jnp.concatenate([left[0, 0], left[0, 1]], axis=1))
    ortho = dot_rows(high, xh[...]) + dot_rows(low, xh[...]) + dot_rows(high, xl[...])
    feed = (ortho * (1.0 - ema_decay)).astype(BF16)
    high, low = split(ortho * (scale * rms))
    rows = high.shape[0]
    stack = jnp.concatenate([feed, high, low], axis=0)
    for j in range(tiles):
        at = slice(j * width, (j + 1) * width)
        value = dot(stack, fh[j])
        direction = value[rows : 2 * rows] + value[2 * rows :] + dot(high, fl[j])
        new_mom[0, :, at] = (mom[0, :, at] + grad[0, :, at].astype(F32)) - value[:rows]
        update[0, :, at] = direction.astype(BF16)
    new_q[0] = fact[0, step].T * scale


def output_call(plan, momentum, gradient, left, inverse, fact, square):
    E, R, C, K, H = plan.matrices, plan.rows, plan.cols, plan.rank, plan.half_rank
    T, W = plan.tiles, plan.width
    block = R // T
    rms = math.sqrt(R * plan.fsdp / K)
    tall = pl.BlockSpec((1, block, C), lambda e, i: (e, i, 0))
    return pl.pallas_call(
        functools.partial(output_kernel, rms, float(C * plan.dp)),
        grid=(E, T),
        out_shape=(
            jax.ShapeDtypeStruct((E, R, C), F32),
            jax.ShapeDtypeStruct((E, R, C), BF16),
            jax.ShapeDtypeStruct((E, C, K), F32),
        ),
        in_specs=[
            tall,
            tall,
            pl.BlockSpec((1, 2, block, H), lambda e, i: (e, 0, i, 0)),
            pl.BlockSpec((1, K, K), lambda e, i: (e, 0, 0)),
            pl.BlockSpec((1, T, K, W), lambda e, i: (e, 0, 0, 0)),
            pl.BlockSpec((1, 8, K), lambda e, i: (e, 0, 0)),
        ],
        out_specs=(tall, tall, pl.BlockSpec((1, W, K), lambda e, i: (e, i, 0))),
        scratch_shapes=[
            pltpu.VMEM((T, K, W), BF16),
            pltpu.VMEM((T, K, W), BF16),
            pltpu.VMEM((K, K), BF16),
            pltpu.VMEM((K, K), BF16),
        ],
        compiler_params=pltpu.CompilerParams(vmem_limit_bytes=48 << 20),
        cost_estimate=pl.CostEstimate(
            flops=8 * E * R * C * K, bytes_accessed=12 * E * R * C, transcendentals=0
        ),
        name="dion_outputs",
    )(momentum, gradient, left, inverse, fact, square)


def body(mesh, momentum, gradient, q_factor):
    plan = Plan(mesh, momentum, q_factor)
    if not plan.fits():
        return general_body(momentum, gradient, q_factor)
    left, inverse, fact, square = factor_call(plan, momentum, gradient, q_factor)
    return output_call(plan, momentum, gradient, left, inverse, fact, square)


def solution(mesh):
    placed = (P(None, "fsdp", "dp"), P(None, "fsdp", "dp"), P(None, "dp", None))
    return jax.shard_map(
        functools.partial(body, mesh),
        mesh=mesh,
        in_specs=placed,
        out_specs=(P(None, "fsdp", "dp"), P(None, "fsdp", "dp"), P(None, "dp", None)),
        check_vma=False,
    )
```

```python
import functools
import math

import jax
import jax.numpy as jnp
from jax import lax
from jax.experimental import pallas as pl
from jax.experimental.pallas import tpu as pltpu
from jax.sharding import PartitionSpec as P

MESH = pl.DeviceIdType.MESH
F32 = jnp.float32
BF16 = jnp.bfloat16

ema_decay = 0.75
epsilon = 1e-06
BLOCK = 128
FULL = lax.Precision.HIGHEST
THREE = lax.Precision.HIGH
ONE = lax.Precision.DEFAULT


def inverse_factor_kernel(gram_ref, out_ref, work_left, work_right):
    matrices, size, _ = gram_ref.shape
    rows = lax.broadcasted_iota(jnp.int32, (size, 1), 0)
    lanes = lax.broadcasted_iota(jnp.int32, (1, size), 1)
    eye = jnp.where(rows == lanes, 1.0, 0.0).astype(jnp.float32)
    for e in range(matrices):
        work_left[e] = gram_ref[e]
        work_right[e] = eye

    def step(k, carry):
        for e in range(matrices):
            left = work_left[e]
            right = work_right[e]
            row_left = work_left[e, pl.ds(k, 1), :]
            row_right = work_right[e, pl.ds(k, 1), :]
            pivot = jnp.sum(jnp.where(lanes == k, row_left, 0.0), axis=1, keepdims=True)
            inverse = lax.rsqrt(pivot)
            row_left = row_left * inverse
            row_right = row_right * inverse
            column = jnp.sum(jnp.where(lanes == k, left, 0.0), axis=1, keepdims=True)
            column = jnp.where(rows > k, column * inverse, 0.0)
            work_left[e] = left - column * row_left
            work_right[e] = jnp.where(rows == k, row_right, right - column * row_right)
        return carry

    lax.fori_loop(0, size, step, 0)
    for e in range(matrices):
        out_ref[e] = work_right[e]


def inverse_factor(gram):
    matrices, size, _ = gram.shape
    if size > BLOCK:
        half = size // 2
        top = inverse_factor(gram[:, :half, :half])
        low = jnp.einsum("eij,ekj->eik", gram[:, half:, :half], top, precision=FULL)
        rest = gram[:, half:, half:] - jnp.einsum("eij,ekj->eik", low, low, precision=FULL)
        bottom = inverse_factor(rest)
        cross = -jnp.einsum(
            "eij,ejk->eik", bottom, jnp.einsum("eij,ejk->eik", low, top, precision=FULL), precision=FULL
        )
        zero = jnp.zeros_like(cross).swapaxes(1, 2)
        return jnp.concatenate(
            [jnp.concatenate([top, zero], 2), jnp.concatenate([cross, bottom], 2)], 1
        )
    return pl.pallas_call(
        inverse_factor_kernel,
        out_shape=jax.ShapeDtypeStruct(gram.shape, jnp.float32),
        in_specs=[pl.BlockSpec(memory_space=pltpu.VMEM)],
        out_specs=pl.BlockSpec(memory_space=pltpu.VMEM),
        scratch_shapes=[pltpu.VMEM((matrices, size, size), jnp.float32)] * 2,
        cost_estimate=pl.CostEstimate(
            flops=size * size * size * 4 * matrices, bytes_accessed=8 * size * size * matrices, transcendentals=0
        ),
        name="inverse_factor",
    )(gram)


def swap(value, axis, mask):
    size = lax.axis_size(axis)
    return lax.ppermute(value, axis, [(i, i ^ mask) for i in range(size)])


def levels_of(size):
    return [(1, 0) if i == 0 else ((2 << i) - 2, i) for i in range(size.bit_length() - 1)]


def side_of(index, bit):
    if bit == 0:
        return index & 1
    return ((index >> bit) ^ (index >> (bit + 1))) & 1


def keep_half(value, axis, mask, side):
    half = value.shape[0] // 2
    own = lax.dynamic_slice_in_dim(value, side * half, half, 0)
    other = lax.dynamic_slice_in_dim(value, (1 - side) * half, half, 0)
    return own + swap(other, axis, mask)


def both_halves(value, axis, mask, side):
    other = swap(value, axis, mask)
    return jnp.where(
        side == 0, jnp.concatenate([value, other], 0), jnp.concatenate([other, value], 0)
    )


def sum_halving(value, axis, levels):
    index = lax.axis_index(axis)
    for mask, bit in levels:
        value = keep_half(value, axis, mask, side_of(index, bit))
    for mask, bit in reversed(levels):
        value = both_halves(value, axis, mask, side_of(index, bit))
    return value


def sum_doubling(value, axis, levels):
    for mask, _ in levels:
        value = value + swap(value, axis, mask)
    return value


def sum_near_first(value, axis, levels):
    index = lax.axis_index(axis)
    mask, bit = levels[0]
    side = side_of(index, bit)
    value = keep_half(value, axis, mask, side)
    value = sum_doubling(value, axis, levels[1:])
    return both_halves(value, axis, mask, side)


def general_body(momentum, gradient, q_factor):
    matrices, local_rows, local_cols = momentum.shape
    rank_width = q_factor.shape[2]
    total_rows = local_rows * lax.axis_size("fsdp")
    total_cols = local_cols * lax.axis_size("dp")
    dp_levels = levels_of(lax.axis_size("dp"))
    fsdp_levels = levels_of(lax.axis_size("fsdp"))
    buffers = [momentum[e] + gradient[e].astype(jnp.float32) for e in range(matrices)]
    lefts, grams, rights = [], [], []
    for e in range(matrices):
        partial_value = jnp.einsum("cn,nr->cr", buffers[e], q_factor[e], precision=THREE)
        order = dp_levels if e % 2 == 0 else dp_levels[1:2] + dp_levels[:1] + dp_levels[2:]
        left = sum_halving(partial_value, "dp", order)
        gram = jnp.einsum("cr,ck->rk", left, left, precision=FULL)
        lefts.append(left)
        grams.append(sum_doubling(gram, "fsdp", fsdp_levels))
        right_raw = jnp.einsum("cn,cr->nr", buffers[e], left, precision=THREE)
        rights.append(sum_near_first(right_raw, "fsdp", fsdp_levels))
    inverse = inverse_factor(jnp.stack(grams))
    orthos = [jnp.einsum("cr,kr->ck", lefts[e], inverse[e], precision=FULL) for e in range(matrices)]
    factors = [jnp.einsum("nr,kr->nk", rights[e], inverse[e], precision=FULL) for e in range(matrices)]
    squares = jnp.stack([jnp.sum(f * f, axis=0) for f in factors])
    squares = sum_doubling(squares, "dp", dp_levels)
    col_scale = lax.rsqrt(squares / total_cols + epsilon)
    rms = jnp.sqrt(jnp.float32(total_rows) / jnp.float32(rank_width))
    momenta, updates, new_qs = [], [], []
    for e in range(matrices):
        feedback = jnp.einsum("cr,nr->cn", orthos[e], factors[e], precision=ONE)
        momenta.append(buffers[e] - (1.0 - ema_decay) * feedback)
        new_q = factors[e] * col_scale[e][None, :]
        new_qs.append(new_q)
        direction = jnp.einsum("cr,nr->cn", orthos[e] * rms, new_q, precision=THREE)
        updates.append(direction.astype(jnp.bfloat16))
    return (jnp.stack(momenta), jnp.stack(updates), jnp.stack(new_qs))


def split(value):
    high = value.astype(BF16)
    return high, (value - high.astype(F32)).astype(BF16)


def dot(a, b):
    return jnp.dot(a, b, preferred_element_type=F32)


def dot_rows(a, b):
    return lax.dot_general(a, b, (((1,), (1,)), ((), ())), preferred_element_type=F32)


def eliminate(work, size, part):
    top = part * (size // 2)
    lanes = lax.broadcasted_iota(jnp.int32, (1, size), 1)
    rows = lax.broadcasted_iota(jnp.int32, (size - top, 1), 0) + top
    eight = lax.broadcasted_iota(jnp.int32, (8, 1), 0)

    def step(it, carry):
        base = pl.multiple_of(it * 8, 8)
        whole = work[top:, :]
        block = work[pl.ds(base, 8), :]
        columns, pivots = [], []
        for j in range(8):
            here = lanes == base + j
            columns.append(jnp.sum(jnp.where(here, whole[:, :size], 0.0), axis=1, keepdims=True))
            pivots.append(jnp.sum(jnp.where(here, block[:, :size], 0.0), axis=1, keepdims=True))
        scaled, roots = [], []
        for k in range(8):
            root = lax.rsqrt(pivots[k][k : k + 1, :])
            inverse = root * root
            below = jnp.where(eight > k, pivots[k], 0.0)
            row = block[k : k + 1, :] * inverse
            block = block - below * row
            for j in range(k + 1, 8):
                factor = pivots[j][k : k + 1, :] * inverse
                pivots[j] = pivots[j] - below * factor
                columns[j] = columns[j] - columns[k] * factor
            scaled.append(row)
            roots.append(root)
        under = rows >= base + 8
        for k in range(8):
            whole = whole - jnp.where(under, columns[k], 0.0) * scaled[k]
        work[top:, :] = whole
        root = roots[0]
        for k in range(1, 8):
            root = jnp.where(eight == k, roots[k], root)
        work[pl.ds(base, 8), :] = block * root
        return carry

    lax.fori_loop(top // 8, (top + size // 2) // 8, step, 0)


class Plan:
    def __init__(self, mesh, momentum, q_factor):
        self.matrices, self.rows, self.cols = momentum.shape
        self.rank = q_factor.shape[2]
        self.half_rank = self.rank // 2
        self.dp, self.fsdp = mesh.shape["dp"], mesh.shape["fsdp"]
        self.pairs = 4
        self.chunk = self.rows // (2 * self.pairs)
        self.half = self.chunk // 2
        self.width = 256
        self.tiles = self.cols // self.width

    def fits(self):
        return (
            self.dp == 8
            and self.fsdp == 4
            and self.rank == 256
            and self.rows % (32 * self.pairs) == 0
            and self.rows % 128 == 0
            and self.cols % (4 * self.width) == 0
            and self.rows % (16 * self.tiles) == 0
            and self.matrices * self.rows * self.cols <= 6 << 20
        )


def factor_kernel(
    plan,
    mom,
    grad,
    q,
    left_out,
    inverse_out,
    fact_out,
    square_out,
    bh,
    bl,
    mst,
    gst,
    qh,
    ql,
    left,
    final,
    a_y,
    a_z1,
    a_z2,
    b_z1,
    b_z2,
    b_y,
    turned,
    turned_split,
    own,
    from_core,
    from_x,
    right,
    gram0,
    gram_core,
    gram_x,
    work,
    inverse,
    sq,
    sq_in,
    sq_all,
    in_sem,
    q_sem,
    l_send,
    l_recv,
    r_send,
    r_recv,
    g_send,
    g_recv,
    s_send,
    s_recv,
    out_sem,
):
    E, K, H = plan.matrices, plan.rank, plan.half_rank
    NP, CH, HF, W, T = plan.pairs, plan.chunk, plan.half, plan.width, plan.tiles
    R = plan.rows
    d, f = lax.axis_index("dp"), lax.axis_index("fsdp")
    y, z = d % 2, d // 2
    core = f % 2
    mid = jnp.logical_or(z == 1, z == 2)
    leaf = jnp.logical_not(mid)
    zside = z // 2
    y_peer = (z * 2 + 1 - y, f)
    z_peer = ((z + 1 - 2 * (z % 2)) * 2 + y, f)
    m_peer = ((3 - z) * 2 + y, f)
    x_peer = (d, (f + 2) % 4)
    c_peer = (d, f + 1 - 2 * core)

    def remote(src, dst, send, recv, peer):
        return pltpu.make_async_remote_copy(
            src_ref=src, dst_ref=dst, send_sem=send, recv_sem=recv, device_id=peer, device_id_type=MESH
        )

    PR, CS = 2 * CH, plan.cols // 2

    def load(n, side):
        e, at = n // NP, pl.ds(pl.multiple_of(lax.rem(n, NP) * PR, PR), PR)
        cs = pl.ds(side * CS, CS)
        return (
            pltpu.make_async_copy(mom.at[e, at, cs], mst.at[side], in_sem.at[0, side]),
            pltpu.make_async_copy(grad.at[e, at, cs], gst.at[side], in_sem.at[1, side]),
        )

    def load_q(e):
        return [
            pltpu.make_async_copy(q.at[e, pl.ds(j * W, W), :], right.at[E - 1, j], q_sem.at[j]) for j in range(T)
        ]

    for copy in load_q(0):
        copy.start()
    for slot in range(2):
        for copy in load(0, slot):
            copy.start()

    barrier = pltpu.get_barrier_semaphore()
    others = [(lax.rem(d + i, plan.dp), f) for i in range(1, plan.dp)]
    for peer in (*others, x_peer, c_peer):
        pl.semaphore_signal(barrier, inc=1, device_id=peer, device_id_type=MESH)

    def left_pair(n):
        e, p = n // NP, lax.rem(n, NP)

        @pl.when(p == 0)
        def _():
            for j, copy in enumerate(load_q(e)):
                copy.wait()
                high, low = split(right[E - 1, j])
                qh[j * W : (j + 1) * W, :] = high
                ql[j * W : (j + 1) * W, :] = low

            @pl.when(e + 1 < E)
            def _():
                for copy in load_q(e + 1):
                    copy.start()

        at = pl.ds(pl.multiple_of(p * PR, PR), PR)
        for side in range(2):
            for copy in load(n, side):
                copy.wait()
            total = jnp.zeros((PR, K), F32)
            for c in range(0, CS, 256):
                cs, ks = slice(c, c + 256), slice(side * CS + c, side * CS + c + 256)
                high, low = split(mst[side, :, cs] + gst[side, :, cs].astype(F32))
                bh[e, at, ks] = high
                bl[e, at, ks] = low
                both = dot(jnp.concatenate([high, low], axis=0), qh[ks, :])
                total = total + (both[:PR] + both[PR:] + dot(high, ql[ks, :]))

            @pl.when(n + 1 < E * NP)
            def _():
                for copy in load(n + 1, side):
                    copy.start()

            for h in range(2):
                part = total[:, h * H : (h + 1) * H]
                left[e * 2 + h, at, :] = part if side == 0 else left[e * 2 + h, at, :] + part

    def rows_of(color, p, part=None):
        base = (2 * p + color) * CH
        if part is None:
            return pl.ds(pl.multiple_of(base, CH), CH)
        return pl.ds(pl.multiple_of(base + part * HF, HF), HF)

    def copies(k):
        unit, p = k // NP, lax.rem(k, NP)
        s, r = (lambda i: l_send.at[k, i]), (lambda i: l_recv.at[k, i])
        part = lambda ref, color, which=None: ref.at[unit, rows_of(color, p, which), :]
        mine, other = part(left, 0, y), part(left, 0, 1 - y)
        done, done_other = part(final, 0, y), part(final, 0, 1 - y)
        zmine, zother = part(left, 1, zside), part(left, 1, 1 - zside)
        zdone, zdone_other = part(final, 1, zside), part(final, 1, 1 - zside)
        made = dict(
            a0=(other, a_y.at[k], s(0), r(0), y_peer),
            a1=(mine, a_z1.at[k], s(1), r(1), z_peer),
            a2=(mine, a_z2.at[k], s(1), r(2), m_peer),
            a3=(done, done, s(2), r(1), z_peer),
            a4=(done, done, s(3), r(3), y_peer),
            a5=(done_other, done_other, s(3), r(3), y_peer),
            b0=(part(left, 1), b_z1.at[k], s(4), r(4), z_peer),
            b1=(zother, b_z2.at[k], s(4), r(5), m_peer),
            b2=(zmine, b_y.at[k], s(5), r(6), y_peer),
            b3=(zdone, zdone, s(6), r(7), m_peer),
            b3w=(zdone_other, zdone_other, s(6), r(7), m_peer),
            b4=(zdone, zdone, s(7), r(4), z_peer),
            b5=(zdone_other, zdone_other, s(8), r(5), z_peer),
        )
        return lambda name: remote(*made[name])

    def stage(k, s):
        unit, p = k // NP, lax.rem(k, NP)
        c = copies(k)
        at = lambda color, part=None: (unit, rows_of(color, p, part), slice(None))
        if s == 0:
            c("a0").start()
            pl.when(leaf)(c("b0").start)
        elif s == 1:
            c("a0").wait_recv()
            left[at(0, y)] = left[at(0, y)] + a_y[k]

            @pl.when(leaf)
            def _():
                c("a1").start()

            @pl.when(mid)
            def _():
                c("b0").wait_recv()
                left[at(1)] = left[at(1)] + b_z1[k]
                c("b1").start()
        elif s == 2:

            @pl.when(mid)
            def _():
                c("a1").wait_recv()
                left[at(0, y)] = left[at(0, y)] + a_z1[k]
                c("a2").start()
                c("b1").wait_recv()
                left[at(1, zside)] = left[at(1, zside)] + b_z2[k]
                c("b2").start()
        elif s == 3:

            @pl.when(mid)
            def _():
                c("a2").wait_recv()
                final[at(0, y)] = left[at(0, y)] + a_z2[k]
                c("a3").start()
                c("a4").start()
                c("b2").wait_recv()
                final[at(1, zside)] = left[at(1, zside)] + b_y[k]
                c("b3").start()
                c("b4").start()
        elif s == 4:

            @pl.when(leaf)
            def _():
                c("a3").wait_recv()
                c("a4").start()

            @pl.when(mid)
            def _():
                c("b3w").wait_recv()
                c("b5").start()
        elif s == 5:
            c("a5").wait_recv()

            @pl.when(leaf)
            def _():
                c("b4").wait_recv()
                c("b5").wait_recv()

    SLOTS, STAGES, DELAYS = E * 2 * NP, 6, (0, 2, 3, 4, 5, 6)

    def slot(t):
        for s in reversed(range(STAGES)):
            k = t - DELAYS[s]
            pl.when(jnp.logical_and(k >= 0, k < SLOTS))(functools.partial(stage, k, s))

    def drain(k):
        c = copies(k)
        c("a0").wait_send()
        c("a4").wait_send()

        @pl.when(leaf)
        def _():
            c("b0").wait_send()
            c("a1").wait_send()

        @pl.when(mid)
        def _():
            for name in ("b1", "a2", "b2", "a3", "b3", "b4", "b5"):
                c(name).wait_send()

    def write_left(u):
        return pltpu.make_async_copy(final.at[u], left_out.at[u // 2, lax.rem(u, 2)], out_sem.at[u // 2, lax.rem(u, 2)])

    def gram_copy(u, which):
        src, dst = ((gram0, gram_core), (gram_core, gram_x))[which]
        peer = (c_peer, x_peer)[which]
        return remote(src.at[u], dst.at[u], g_send.at[u, which], g_recv.at[u, which], peer)

    def turn(u):
        write_left(u).start()
        for c in range(0, R, 128):
            turned[:, c : c + 128] = final[u, c : c + 128, :].T

        high, low = split(turned[...])
        turned_split[:H, :] = high
        turned_split[H:, :] = low

    def gram_first(u):
        e, h = u // 2, lax.rem(u, 2)

        def block(j, at):
            gram0[u, :, at] = jnp.dot(turned[...], final[e * 2 + j], precision=FULL, preferred_element_type=F32)

        block(0, slice(0, H))
        pl.when(h == 1)(lambda: block(1, slice(H, K)))

        @pl.when(h == 0)
        def _():
            gram0[u, :, H:] = jnp.zeros((H, K - H), F32)

        gram_copy(u, 0).start()

    def gram_second(u):
        gram_copy(u, 0).wait_recv()
        gram_core[u] = gram0[u] + gram_core[u]
        gram_copy(u, 1).start()

    def gram_third(u):
        gram_copy(u, 1).wait_recv()
        gram_x[u] = gram_core[u] + gram_x[u]

    def full(a, b, rows=False):
        if rows:
            return lax.dot_general(a, b, (((1,), (1,)), ((), ())), precision=FULL, preferred_element_type=F32)
        return jnp.dot(a, b, precision=FULL, preferred_element_type=F32)

    def factor_first(u):
        e, h = u // 2, lax.rem(u, 2)
        eye = jnp.where(
            lax.broadcasted_iota(jnp.int32, (H, H), 0) == lax.broadcasted_iota(jnp.int32, (H, H), 1), 1.0, 0.0
        ).astype(F32)
        work[:, H:] = eye

        @pl.when(h == 0)
        def _():
            work[:, :H] = gram_x[u, :, :H]

        @pl.when(h == 1)
        def _():
            top = inverse[e, :H, :H]
            low = full(gram_x[u, :, :H], top, rows=True)
            work[:, :H] = gram_x[u, :, H:] - full(low, low, rows=True)
            inverse[e, H:, :H] = full(low, top)

        eliminate(work, H, 0)

    def factor_second(u):
        e, h = u // 2, lax.rem(u, 2)
        eliminate(work, H, 1)

        @pl.when(h == 0)
        def _():
            inverse[e, :H, :H] = work[:, H:]
            inverse[e, :H, H:] = jnp.zeros((H, K - H), F32)

        @pl.when(h == 1)
        def _():
            bottom = work[:, H:]
            inverse[e, H:, H:] = bottom
            inverse[e, H:, :H] = -full(bottom, inverse[e, H:, :H])

    def right_copy(u, s, which):
        e, h = u // 2, lax.rem(u, 2)
        tile, other = 2 * s + core, 2 * s + 1 - core
        hs = pl.ds(pl.multiple_of(h * H, H), H)
        if which == 0:
            src, dst, peer = own.at[u, other], from_core.at[u, s], c_peer
        elif which == 1:
            src, dst, peer = own.at[u, tile], from_x.at[u, s], x_peer
        else:
            tile = tile if which == 2 else other
            src = dst = right.at[e, tile, hs, :]
            peer, which = c_peer, 2
        return remote(src, dst, r_send.at[u, s, which], r_recv.at[u, s, which], peer)

    def right_forward(u, s):
        right_copy(u, s, 0).wait_recv()
        tile = 2 * s + core
        own[u, tile] = own[u, tile] + from_core[u, s]
        right_copy(u, s, 1).start()

    def right_product(u, s):
        e = u // 2
        for i in range(2):
            at = pl.ds(pl.multiple_of((s * 2 + i) * W, W), W)
            both = dot(turned_split[...], bh[e, :, at])
            own[u, 2 * s + i] = both[:H] + both[H:] + dot(turned_split[:H, :], bl[e, :, at])
        right_copy(u, s, 0).start()

    def right_sums(u):
        e, h = u // 2, lax.rem(u, 2)
        for s in range(T // 2):
            right_copy(u, s, 1).wait_recv()
            tile = 2 * s + core
            right[e, tile, pl.ds(pl.multiple_of(h * H, H), H), :] = own[u, tile] + from_x[u, s]
            right_copy(u, s, 2).start()

    def right_others(u):
        for s in range(T // 2):
            right_copy(u, s, 3).wait_recv()

    def write_fact(e, j):
        return pltpu.make_async_copy(right.at[e, j], fact_out.at[e, j], out_sem.at[e, 2 + j])

    def write_inverse(e):
        return pltpu.make_async_copy(inverse.at[e], inverse_out.at[e], out_sem.at[e, 2 + T])

    def write_square(e):
        return pltpu.make_async_copy(sq_all.at[e], square_out.at[e], out_sem.at[e, 3 + T])

    def square_copy(e, i):
        peer = lax.rem(d + i, plan.dp)
        return remote(sq.at[e], sq_in.at[e, d], s_send.at[e, i - 1], s_recv.at[e, i - 1], (peer, f))

    def square_arrival(e, i):
        source = lax.rem(d + plan.dp - i, plan.dp)
        return remote(sq.at[e], sq_in.at[e, source], s_send.at[e, i - 1], s_recv.at[e, i - 1], (source, f))

    def factors(e):
        write_inverse(e).start()
        for s in range(T // 2):
            right_copy(e * 2, s, 2).wait_send()
            right_copy(e * 2 + 1, s, 2).wait_send()
        x_high, x_low = split(inverse[e])
        total = jnp.zeros((K, 128), F32)
        for j in range(T):
            high, low = split(right[e, j])
            value = dot(x_high, high) + dot(x_low, high) + dot(x_high, low)
            right[e, j] = value
            write_fact(e, j).start()
            for c in range(0, W, 128):
                total = total + value[:, c : c + 128] * value[:, c : c + 128]
        row = jnp.sum(total.T, axis=0, keepdims=True)
        sq[e] = jnp.broadcast_to(row, (8, K))
        for i in range(1, plan.dp):
            square_copy(e, i).start()
        sq_in[e, d] = sq[e]

    def square_sum(e):
        for i in range(1, plan.dp):
            square_arrival(e, i).wait_recv()
        total = sq_in[e, 0]
        for i in range(1, plan.dp):
            total = total + sq_in[e, i]
        sq_all[e] = total
        write_square(e).start()

    left_pair(0)
    pl.semaphore_wait(barrier, plan.dp + 1)
    slot(0)

    def early(t, carry):
        left_pair(t)
        slot(t)
        return carry

    lax.fori_loop(1, E * NP, early, 0)

    FIRST = NP - 1 + DELAYS[-1]
    lax.fori_loop(E * NP, FIRST, lambda t, carry: (slot(t), carry)[1], 0)

    def late(u, carry):
        t = FIRST + u * NP
        slot(t)
        turn(u)
        gram_first(u)
        right_product(u, 0)
        gram_second(u)
        right_product(u, 1)
        right_forward(u, 0)
        slot(t + 1)
        for s in range(2, T // 2):
            right_product(u, s)
            right_forward(u, s - 1)
        slot(t + 2)
        right_forward(u, T // 2 - 1)
        gram_third(u)
        factor_first(u)
        slot(t + 3)
        pl.when(u > 0)(lambda: right_sums(u - 1))
        factor_second(u)

        @pl.when(u == 2)
        def _():
            right_others(0)
            right_others(1)
            factors(0)

        return carry

    lax.fori_loop(0, E * 2, late, 0)
    right_sums(E * 2 - 1)
    right_others(E * 2 - 2)
    right_others(E * 2 - 1)
    factors(E - 1)
    square_sum(0)
    square_sum(E - 1)

    lax.fori_loop(0, SLOTS, lambda k, carry: (drain(k), carry)[1], 0)

    def close(u, carry):
        for s in range(T // 2):
            right_copy(u, s, 0).wait_send()
            right_copy(u, s, 1).wait_send()
        gram_copy(u, 0).wait_send()
        gram_copy(u, 1).wait_send()
        write_left(u).wait()
        return carry

    lax.fori_loop(0, E * 2, close, 0)
    for e in range(E):
        for i in range(1, plan.dp):
            square_copy(e, i).wait_send()
        for j in range(T):
            write_fact(e, j).wait()
        write_inverse(e).wait()
        write_square(e).wait()


def factor_call(plan, momentum, gradient, q_factor):
    E, R, C, K, H = plan.matrices, plan.rows, plan.cols, plan.rank, plan.half_rank
    NP, CH, HF, W, T = plan.pairs, plan.chunk, plan.half, plan.width, plan.tiles
    U = E * 2 * NP
    any_spec = pl.BlockSpec(memory_space=pl.ANY)
    vmem = pltpu.VMEM
    flops = 14 * E * R * C * K
    return pl.pallas_call(
        functools.partial(factor_kernel, plan),
        out_shape=(
            jax.ShapeDtypeStruct((E, 2, R, H), F32),
            jax.ShapeDtypeStruct((E, K, K), F32),
            jax.ShapeDtypeStruct((E, T, K, W), F32),
            jax.ShapeDtypeStruct((E, 8, K), F32),
        ),
        in_specs=[any_spec] * 3,
        out_specs=(any_spec,) * 4,
        scratch_shapes=[
            vmem((E, R, C), BF16),
            vmem((E, R, C), BF16),
            vmem((2, 2 * CH, C // 2), F32),
            vmem((2, 2 * CH, C // 2), BF16),
            vmem((C, K), BF16),
            vmem((C, K), BF16),
            vmem((E * 2, R, H), F32),
            vmem((E * 2, R, H), F32),
            vmem((U, HF, H), F32),
            vmem((U, HF, H), F32),
            vmem((U, HF, H), F32),
            vmem((U, CH, H), F32),
            vmem((U, HF, H), F32),
            vmem((U, HF, H), F32),
            vmem((H, R), F32),
            vmem((K, R), BF16),
            vmem((E * 2, T, H, W), F32),
            vmem((E * 2, T // 2, H, W), F32),
            vmem((E * 2, T // 2, H, W), F32),
            vmem((E, T, K, W), F32),
            vmem((E * 2, H, K), F32),
            vmem((E * 2, H, K), F32),
            vmem((E * 2, H, K), F32),
            vmem((H, K), F32),
            vmem((E, K, K), F32),
            vmem((E, 8, K), F32),
            vmem((E, plan.dp, 8, K), F32),
            vmem((E, 8, K), F32),
            pltpu.SemaphoreType.DMA((2, 2)),
            pltpu.SemaphoreType.DMA((T,)),
            pltpu.SemaphoreType.DMA((U, 9)),
            pltpu.SemaphoreType.DMA((U, 8)),
            pltpu.SemaphoreType.DMA((E * 2, T // 2, 3)),
            pltpu.SemaphoreType.DMA((E * 2, T // 2, 3)),
            pltpu.SemaphoreType.DMA((E * 2, 2)),
            pltpu.SemaphoreType.DMA((E * 2, 2)),
            pltpu.SemaphoreType.DMA((E, plan.dp - 1)),
            pltpu.SemaphoreType.DMA((E, plan.dp - 1)),
            pltpu.SemaphoreType.DMA((E, T + 4)),
        ],
        compiler_params=pltpu.CompilerParams(
            collective_id=0, has_side_effects=True, vmem_limit_bytes=67043328
        ),
        cost_estimate=pl.CostEstimate(flops=flops, bytes_accessed=6 * E * R * C, transcendentals=0),
        name="dion_factors",
    )(momentum, gradient, q_factor)


def output_kernel(
    rms, total_cols, parts, mom, grad, left, inverse, fact, square, new_mom, update, new_q, fh, fl, xh, xl
):
    tiles, width = fact.shape[1], fact.shape[3]
    step = pl.program_id(1)

    @pl.when(step == 0)
    def _():
        for j in range(tiles):
            high, low = split(fact[0, j])
            fh[j] = high
            fl[j] = low
        high, low = split(inverse[0])
        xh[...] = high
        xl[...] = low

    scale = lax.rsqrt(square[0, 0:1, :] / total_cols + epsilon)
    rows = mom.shape[1] // parts

    def piece(i, carry):
        at_rows = pl.ds(pl.multiple_of(i * rows, rows), rows)
        high, low = split(jnp.concatenate([left[0, 0, at_rows, :], left[0, 1, at_rows, :]], axis=1))
        ortho = dot_rows(high, xh[...]) + dot_rows(low, xh[...]) + dot_rows(high, xl[...])
        feed = (ortho * (1.0 - ema_decay)).astype(BF16)
        high, low = split(ortho * (scale * rms))
        stack = jnp.concatenate([feed, high, low], axis=0)
        for j in range(tiles):
            at = slice(j * width, (j + 1) * width)
            value = dot(stack, fh[j])
            direction = value[rows : 2 * rows] + value[2 * rows :] + dot(high, fl[j])
            new_mom[0, at_rows, at] = (mom[0, at_rows, at] + grad[0, at_rows, at].astype(F32)) - value[:rows]
            update[0, at_rows, at] = direction.astype(BF16)
        new_q[0, pl.ds(pl.multiple_of(i * width, width), width), :] = fact[0, step * parts + i].T * scale
        return carry

    lax.fori_loop(0, parts, piece, 0)


def output_call(plan, momentum, gradient, left, inverse, fact, square):
    E, R, C, K, H = plan.matrices, plan.rows, plan.cols, plan.rank, plan.half_rank
    T, W = plan.tiles, plan.width
    parts = 2
    block = R // T * parts
    rms = math.sqrt(R * plan.fsdp / K)
    tall = pl.BlockSpec((1, block, C), lambda e, i: (e, i, 0))
    return pl.pallas_call(
        functools.partial(output_kernel, rms, float(C * plan.dp), parts),
        grid=(E, T // parts),
        out_shape=(
            jax.ShapeDtypeStruct((E, R, C), F32),
            jax.ShapeDtypeStruct((E, R, C), BF16),
            jax.ShapeDtypeStruct((E, C, K), F32),
        ),
        in_specs=[
            tall,
            tall,
            pl.BlockSpec((1, 2, block, H), lambda e, i: (e, 0, i, 0)),
            pl.BlockSpec((1, K, K), lambda e, i: (e, 0, 0)),
            pl.BlockSpec((1, T, K, W), lambda e, i: (e, 0, 0, 0)),
            pl.BlockSpec((1, 8, K), lambda e, i: (e, 0, 0)),
        ],
        out_specs=(tall, tall, pl.BlockSpec((1, W * parts, K), lambda e, i: (e, i, 0))),
        scratch_shapes=[
            pltpu.VMEM((T, K, W), BF16),
            pltpu.VMEM((T, K, W), BF16),
            pltpu.VMEM((K, K), BF16),
            pltpu.VMEM((K, K), BF16),
        ],
        compiler_params=pltpu.CompilerParams(vmem_limit_bytes=67043328),
        cost_estimate=pl.CostEstimate(
            flops=8 * E * R * C * K, bytes_accessed=12 * E * R * C, transcendentals=0
        ),
        name="dion_outputs",
    )(momentum, gradient, left, inverse, fact, square)


def body(mesh, momentum, gradient, q_factor):
    plan = Plan(mesh, momentum, q_factor)
    if not plan.fits():
        return general_body(momentum, gradient, q_factor)
    left, inverse, fact, square = factor_call(plan, momentum, gradient, q_factor)
    return output_call(plan, momentum, gradient, left, inverse, fact, square)


def solution(mesh):
    placed = (P(None, "fsdp", "dp"), P(None, "fsdp", "dp"), P(None, "dp", None))
    return jax.shard_map(
        functools.partial(body, mesh),
        mesh=mesh,
        in_specs=placed,
        out_specs=(P(None, "fsdp", "dp"), P(None, "fsdp", "dp"), P(None, "dp", None)),
        check_vma=False,
    )
```
